32 devices in a mesh: lat: 8 (over z, x), lev: 4 (over y, core).
Axes of the slice: x: 2, y: 2, z: 4, core: 2. Of those that a mesh axis runs over, the one named last changes fastest.
Arguments:
- fourier: bfloat16 [1280, 640, 1024], P('lat', None, 'lev'), may hold values from -6 to 6
- legendre: bfloat16 [640, 2, 640, 320], P('lat', None, 'lev'), may hold values from -0.25 to 0.25
- owner: int32 [640], replicated, may hold values from 0 to 7, as said below
Outputs:
- spectral: bfloat16 [640, 2, 320, 1024], P('lat', None, None, 'lev')
The draws below stay inside these ranges and needn't reach their ends.
Inputs may be any that keep to these rules, and one draw needn't show every extreme that they name: `owner`: each index along lat is named by exactly 80 wavenumbers.
All inputs are finite; a program needn't handle non-finite values.
Results may differ from the reference program's by a relative error of at most 0.0051.
Values may be sent and summed in bfloat16 or wider, within the bound.
No kernel may reach another device: no remote copies, remote signals or barrier semaphores. Data moves between devices by JAX's collectives and lax.ppermute only.
A program may use at most 384 MiB of HBM per device.

```python
import jax
import jax.numpy as jnp
from jax import lax

M = 640
NLAT = 1280
COLS = 1024
NH = 640
HALF = 320
SLOTS = 80
N_LAT = 8


def draw_owner(key, part):
    jitter_key = jax.random.fold_in(key, 101)
    device_key = jax.random.fold_in(key, 202)
    wave_ids = jnp.arange(M, dtype=jnp.int32)
    jitter = jax.random.randint(jitter_key, (M,), 0, 4 * SLOTS, dtype=jnp.int32)
    scores = (wave_ids + jitter) * M + wave_ids
    ordering = jnp.argsort(scores, stable=True).astype(jnp.int32)
    ranking = jnp.argsort(ordering, stable=True).astype(jnp.int32)
    devices = jax.random.permutation(device_key, M // SLOTS).astype(jnp.int32)
    return devices[ranking // SLOTS]


def levels(own_key, extent, split, smallest, high):
    def one(axis_at, shards_of):
        draws = jax.random.uniform(jax.random.fold_in(jax.random.fold_in(own_key, 6), axis_at), (shards_of,), jnp.float32, smallest / len(split), high / len(split))
        return jnp.repeat(jnp.exp(draws), extent[axis_at] // shards_of).reshape((-1,) + (1,) * (len(extent) - axis_at - 1))

    level = one(*split[0])
    for cut in split[1:]:
        level = level * one(*cut)
    return level


def bell_draw(key, dims, scale, reach, shards=(), kind=jnp.bfloat16):
    result = jax.random.normal(key, dims, jnp.float32) * scale
    if len(shards) > 0:
        result = levels(key, dims, shards, -0.22, 0.18) * result
    return jnp.clip(result, min=-reach, max=reach).astype(kind)


def setup_inputs(seed: int = 0) -> dict:
    arg_keys = jax.random.split(jax.random.key(seed), 4)
    fourier = bell_draw(arg_keys[0], (NLAT, M, COLS), 1.0, 6.0, ((0, 8), (2, 4)))
    legendre = bell_draw(arg_keys[1], (M, 2, NH, HALF), NH ** -0.5, 0.25, ((0, 8), (2, 4)))
    owner = draw_owner(jax.random.fold_in(arg_keys[3], 71), 0)
    return {"fourier": fourier, "legendre": legendre, "owner": owner}


def slot_waves(owner, slot_count):
    wave_count = owner.shape[0]
    wave_ids = jnp.arange(wave_count, dtype=jnp.int32)
    earlier = (owner[None, :] == owner[:, None]) & (wave_ids[None, :] < wave_ids[:, None])
    ranked = jnp.sum(earlier.astype(jnp.int32), axis=1)
    placed = owner * slot_count + ranked
    matched = placed[None, :] == wave_ids[:, None]
    return jnp.sum(jnp.where(matched, wave_ids[None, :], 0), axis=1).astype(jnp.int32)


def reference(fourier, legendre, owner):
    wave_of = slot_waves(owner, M // N_LAT)
    north_count = NLAT // 2
    degree = jnp.arange(M // 2, dtype=jnp.int32)
    parities = jnp.arange(2, dtype=jnp.int32)

    def one_slot(operands):
        wave, table_part = operands
        column = lax.dynamic_index_in_dim(fourier, wave, axis=1, keepdims=False)
        upper_rows = column[:north_count].astype(jnp.float32)
        lower_rows = column[north_count:].astype(jnp.float32)
        even_rows = (upper_rows + lower_rows).astype(jnp.bfloat16)
        odd_rows = (upper_rows - lower_rows).astype(jnp.bfloat16)
        even_out = jnp.dot(table_part[0].T, even_rows, preferred_element_type=jnp.float32)
        odd_out = jnp.dot(table_part[1].T, odd_rows, preferred_element_type=jnp.float32)
        live_count = (M - wave - parities + 1) // 2
        kept_mask = degree[None, :] < live_count[:, None]
        stacked = jnp.stack([even_out, odd_out])
        return jnp.where(kept_mask[:, :, None], stacked, 0.0).astype(jnp.bfloat16)

    return lax.map(one_slot, (wave_of, legendre))
```

```python
import functools

import jax
import jax.numpy as jnp
from jax import lax
from jax.experimental import pallas as pl
from jax.experimental.pallas import tpu as pltpu
from jax.sharding import PartitionSpec as P

CHUNK_ENDS = (5, 22, 74, 80)
PICK_GROUP = 4
DEGREE_BLOCK = 128


def slot_waves(owner, slot_count):
    wave_count = owner.shape[0]
    wave_ids = jnp.arange(wave_count, dtype=jnp.int32)
    earlier = (owner[None, :] == owner[:, None]) & (wave_ids[None, :] < wave_ids[:, None])
    ranked = jnp.sum(earlier.astype(jnp.int32), axis=1)
    placed = owner * slot_count + ranked
    matched = placed[None, :] == wave_ids[:, None]
    return jnp.sum(jnp.where(matched, wave_ids[None, :], 0), axis=1)


def chunk_bounds(slot_count):
    ends = {slot_count * end // CHUNK_ENDS[-1] for end in CHUNK_ENDS}
    return sorted(ends | {0})


def pick(wave_ref, *refs):
    out_ref = refs[-1]
    for place, source_ref in enumerate(refs[:-1]):
        out_ref[0, place] = source_ref[0]


def pick_chunk(by_owner, turned, low, high):
    _, rows, columns = turned.shape
    lat_count = by_owner.shape[0]
    chunk = high - low
    group = min(chunk, PICK_GROUP)
    last_wave = by_owner.shape[1] - 1

    def source_of(place):
        def place_of(owner, step, wave_ref):
            slot = jnp.minimum(low + step * group + place, last_wave)
            return wave_ref[owner, slot], 0, 0

        return pl.BlockSpec((1, rows, columns), place_of)

    out = jax.ShapeDtypeStruct((lat_count, chunk, rows, columns), turned.dtype)
    return pl.pallas_call(
        pick,
        out_shape=out,
        grid_spec=pltpu.PrefetchScalarGridSpec(
            num_scalar_prefetch=1,
            grid=(lat_count, pl.cdiv(chunk, group)),
            in_specs=[source_of(place) for place in range(group)],
            out_specs=pl.BlockSpec((1, group, rows, columns), lambda owner, step, wave: (owner, step, 0, 0)),
        ),
        cost_estimate=pl.CostEstimate(flops=0, transcendentals=0, bytes_accessed=4 * out.size),
    )(by_owner, *[turned] * group)


def project(first_slot, counts_ref, source_ref, *rest):
    groups, _, rows, columns = source_ref.shape
    half_groups = groups // 2
    table_refs = rest[:half_groups]
    out_ref = rest[-1]
    _, _, _, degrees = table_refs[0].shape
    slot = first_slot + pl.program_id(0)
    upper, lower = [], []
    for place in range(half_groups):
        block = counts_ref[counts_ref.shape[0] - 1, place]
        upper.append(source_ref[block, 0].astype(jnp.float32))
        lower.append(source_ref[half_groups + block, 0].astype(jnp.float32))
    for parity in range(2):
        pairs = zip(upper, lower)
        parts = [north + south if parity == 0 else north - south for north, south in pairs]
        source = jnp.concatenate([part.astype(jnp.bfloat16) for part in parts], axis=0)
        live = counts_ref[slot, parity]
        for low in range(0, degrees, DEGREE_BLOCK):
            high = min(low + DEGREE_BLOCK, degrees)

            @pl.when(live > low)
            def _(low=low, high=high, source=source, live=live, parity=parity):
                tile = jnp.concatenate([ref[0, parity, :, low:high] for ref in table_refs], axis=0)
                total = lax.dot_general(
                    tile, source, (((0,), (0,)), ((), ())), preferred_element_type=jnp.float32
                )
                degree = low + lax.broadcasted_iota(jnp.int32, total.shape, 0)
                out_ref[0, parity, low:high, :] = jnp.where(degree < live, total, 0.0).astype(out_ref.dtype)

            @pl.when(live <= low)
            def _(low=low, high=high, parity=parity):
                out_ref[0, parity, low:high, :] = jnp.zeros((high - low, columns), out_ref.dtype)


def project_chunk(counts, arrived, tables, spectral, first_slot):
    groups, chunk, rows, columns = arrived.shape
    slot_count, parities, table_rows, degrees = tables[0].shape
    in_specs = [pl.BlockSpec((groups, 1, rows, columns), lambda i, counts: (0, i, 0, 0))]
    for _ in tables:
        in_specs.append(
            pl.BlockSpec((1, parities, table_rows, degrees), lambda i, counts: (first_slot + i, 0, 0, 0))
        )
    operands = [counts, arrived, *tables]
    aliases = {}
    if spectral is not None:
        in_specs.append(pl.BlockSpec(memory_space=pl.ANY))
        aliases = {len(operands): 0}
        operands.append(spectral)
    flops = 2 * chunk * parities * len(tables) * table_rows * degrees * columns
    return pl.pallas_call(
        functools.partial(project, first_slot),
        out_shape=jax.ShapeDtypeStruct((slot_count, parities, degrees, columns), jnp.bfloat16),
        grid_spec=pltpu.PrefetchScalarGridSpec(
            num_scalar_prefetch=1,
            grid=(chunk,),
            in_specs=in_specs,
            out_specs=pl.BlockSpec(
                (1, parities, degrees, columns), lambda i, counts: (first_slot + i, 0, 0, 0)
            ),
        ),
        input_output_aliases=aliases,
        cost_estimate=pl.CostEstimate(flops=flops, transcendentals=0, bytes_accessed=4 * arrived.size),
    )(*operands)


def partner(values, distance, count):
    return lax.ppermute(values, "lev", [(place, place ^ distance) for place in range(count)])


def gather_table(legendre, count):
    tables = [legendre]
    distance = count // 2
    while distance:
        tables += [partner(table, distance, count) for table in tables]
        distance //= 2
    offsets = [0]
    distance = count // 2
    while distance:
        offsets += [offset ^ distance for offset in offsets]
        distance //= 2
    return tables, [lax.axis_index("lev") ^ offset for offset in offsets]


def body(fourier, legendre, owner):
    lat_count = lax.axis_size("lat")
    lev_count = lax.axis_size("lev")
    row_count, wave_count, column_count = fourier.shape
    slot_count = wave_count // lat_count
    table_rows = legendre.shape[2]
    wave_of = slot_waves(owner, slot_count)
    by_owner = wave_of.reshape(lat_count, slot_count)
    bounds = chunk_bounds(slot_count)
    chunks = list(zip(bounds[:-1], bounds[1:]))
    turned = None
    arrivals = []
    spectral = None
    done = 0

    def project_next(done, spectral):
        return project_chunk(counts, arrivals[done], tables, spectral, chunks[done][0])

    for index, (low, high) in enumerate(chunks):
        if index == 0:
            waves = by_owner[:, low:high].reshape(-1)
            taken = fourier.at[:, waves, :].get(mode="promise_in_bounds")
            outgoing = jnp.swapaxes(taken, 0, 1).reshape(lat_count, high - low, row_count, column_count)
            outgoing, source, table = lax.optimization_barrier((outgoing, fourier, legendre))
            turned = jnp.swapaxes(source, 0, 1)
            tables, blocks = gather_table(table, lev_count)
            own_waves = lax.dynamic_slice_in_dim(wave_of, lax.axis_index("lat") * slot_count, slot_count)
            parities = jnp.arange(2, dtype=jnp.int32)
            live_count = (wave_count - own_waves[:, None] - parities[None, :] + 1) // 2
            width = max(2, lev_count)
            counts = jnp.zeros((slot_count + 1, width), jnp.int32)
            counts = counts.at[:slot_count, :2].set(live_count)
            counts = counts.at[slot_count, :lev_count].set(jnp.stack(blocks))
        else:
            outgoing = pick_chunk(by_owner, turned, low, high)
        if index == len(chunks) - 1:
            while done < index - 1:
                spectral = project_next(done, spectral)
                done += 1
            if done:
                outgoing, spectral = lax.optimization_barrier((outgoing, spectral))
        arrived = lax.all_to_all(outgoing, "lat", split_axis=0, concat_axis=0, tiled=True)
        if row_count != table_rows:
            arrived = jnp.swapaxes(arrived, 0, 1).reshape(high - low, -1, table_rows, column_count)
            arrived = jnp.swapaxes(arrived, 0, 1)
        arrivals.append(arrived)
    while done < len(chunks):
        spectral = project_next(done, spectral)
        done += 1
    return spectral


def solution(mesh):
    placed = (P("lat", None, "lev"), P("lat", None, "lev", None), P())
    return jax.shard_map(
        body, mesh=mesh, in_specs=placed, out_specs=P("lat", None, None, "lev"), check_vma=False
    )
```

```python
import functools

import jax
import jax.numpy as jnp
from jax import lax
from jax.experimental import pallas as pl
from jax.experimental.pallas import tpu as pltpu
from jax.sharding import PartitionSpec as P


CHUNK_ENDS = (5, 22, 74, 80)
SWAP_ENDS = (4, 12, 58, 74, 78, 80)
PROJECT_GROUP = 2
PICK_GROUP = 4
DEGREE_BLOCK = 128


def slot_waves(owner, slot_count):
    wave_count = owner.shape[0]
    wave_ids = jnp.arange(wave_count, dtype=jnp.int32)
    earlier = (owner[None, :] == owner[:, None]) & (wave_ids[None, :] < wave_ids[:, None])
    ranked = jnp.sum(earlier.astype(jnp.int32), axis=1)
    placed = owner * slot_count + ranked
    matched = placed[None, :] == wave_ids[:, None]
    return jnp.sum(jnp.where(matched, wave_ids[None, :], 0), axis=1)


def chunk_bounds(slot_count, chunk_ends=CHUNK_ENDS):
    ends = {slot_count * end // chunk_ends[-1] for end in chunk_ends}
    return sorted(ends | {0})


def pick(wave_ref, *refs):
    out_ref = refs[-1]
    for place, source_ref in enumerate(refs[:-1]):
        out_ref[0, place] = source_ref[0]


def pick_chunk(by_owner, turned, low, high):
    _, rows, columns = turned.shape
    lat_count = by_owner.shape[0]
    chunk = high - low
    group = min(chunk, PICK_GROUP)
    last_wave = by_owner.shape[1] - 1

    def source_of(place):
        def place_of(owner, step, wave_ref):
            slot = jnp.minimum(low + step * group + place, last_wave)
            return wave_ref[owner, slot], 0, 0

        return pl.BlockSpec((1, rows, columns), place_of)

    out = jax.ShapeDtypeStruct((lat_count, chunk, rows, columns), turned.dtype)
    return pl.pallas_call(
        pick,
        out_shape=out,
        grid_spec=pltpu.PrefetchScalarGridSpec(
            num_scalar_prefetch=1,
            grid=(lat_count, pl.cdiv(chunk, group)),
            in_specs=[source_of(place) for place in range(group)],
            out_specs=pl.BlockSpec((1, group, rows, columns), lambda owner, step, wave: (owner, step, 0, 0)),
        ),
        cost_estimate=pl.CostEstimate(flops=0, transcendentals=0, bytes_accessed=4 * out.size),
    )(by_owner, *[turned] * group)


def project(first_slot, counts_ref, source_ref, *rest):
    groups, _, _, columns = source_ref.shape
    half_groups = groups // 2
    table_refs = rest[:half_groups]
    out_ref = rest[-1]
    _, _, _, degrees = table_refs[0].shape
    slot = first_slot + pl.program_id(0)
    upper, lower = [], []
    for place in range(half_groups):
        block = counts_ref[counts_ref.shape[0] - 1, place]
        upper.append(source_ref[block, 0].astype(jnp.float32))
        lower.append(source_ref[half_groups + block, 0].astype(jnp.float32))
    for parity in range(2):
        pairs = zip(upper, lower)
        parts = [north + south if parity == 0 else north - south for north, south in pairs]
        source = jnp.concatenate([part.astype(jnp.bfloat16) for part in parts], axis=0)
        live = counts_ref[slot, parity]
        for low in range(0, degrees, DEGREE_BLOCK):
            high = min(low + DEGREE_BLOCK, degrees)

            @pl.when(live > low)
            def _(low=low, high=high, source=source, live=live, parity=parity):
                tile = jnp.concatenate([ref[0, parity, :, low:high] for ref in table_refs], axis=0)
                total = lax.dot_general(
                    tile, source, (((0,), (0,)), ((), ())), preferred_element_type=jnp.float32
                )
                degree = low + lax.broadcasted_iota(jnp.int32, total.shape, 0)
                out_ref[0, parity, low:high, :] = jnp.where(degree < live, total, 0.0).astype(out_ref.dtype)

            @pl.when(live <= low)
            def _(low=low, high=high, parity=parity):
                out_ref[0, parity, low:high, :] = jnp.zeros((high - low, columns), out_ref.dtype)


def project_chunk(counts, arrived, tables, spectral, first_slot):
    groups, chunk, rows, columns = arrived.shape
    slot_count, parities, table_rows, degrees = tables[0].shape
    in_specs = [pl.BlockSpec((groups, 1, rows, columns), lambda i, counts: (0, i, 0, 0))]
    for _ in tables:
        in_specs.append(
            pl.BlockSpec((1, parities, table_rows, degrees), lambda i, counts: (first_slot + i, 0, 0, 0))
        )
    operands = [counts, arrived, *tables]
    aliases = {}
    if spectral is not None:
        in_specs.append(pl.BlockSpec(memory_space=pl.ANY))
        aliases = {len(operands): 0}
        operands.append(spectral)
    flops = 2 * chunk * parities * len(tables) * table_rows * degrees * columns
    return pl.pallas_call(
        functools.partial(project, first_slot),
        out_shape=jax.ShapeDtypeStruct((slot_count, parities, degrees, columns), jnp.bfloat16),
        grid_spec=pltpu.PrefetchScalarGridSpec(
            num_scalar_prefetch=1,
            grid=(chunk,),
            in_specs=in_specs,
            out_specs=pl.BlockSpec(
                (1, parities, degrees, columns), lambda i, counts: (first_slot + i, 0, 0, 0)
            ),
        ),
        input_output_aliases=aliases,
        cost_estimate=pl.CostEstimate(flops=flops, transcendentals=0, bytes_accessed=4 * arrived.size),
    )(*operands)


def partner(values, distance, count):
    return lax.ppermute(values, "lev", [(place, place ^ distance) for place in range(count)])


def gather_table(legendre, count):
    tables = [legendre]
    distance = count // 2
    while distance:
        tables += [partner(table, distance, count) for table in tables]
        distance //= 2
    offsets = [0]
    distance = count // 2
    while distance:
        offsets += [offset ^ distance for offset in offsets]
        distance //= 2
    return tables, [lax.axis_index("lev") ^ offset for offset in offsets]


def exchange_body(fourier, legendre, owner):
    lat_count = lax.axis_size("lat")
    lev_count = lax.axis_size("lev")
    row_count, wave_count, column_count = fourier.shape
    slot_count = wave_count // lat_count
    table_rows = legendre.shape[2]
    wave_of = slot_waves(owner, slot_count)
    by_owner = wave_of.reshape(lat_count, slot_count)
    bounds = chunk_bounds(slot_count)
    chunks = list(zip(bounds[:-1], bounds[1:]))
    turned = None
    arrivals = []
    spectral = None
    done = 0

    def project_next(done, spectral):
        return project_chunk(counts, arrivals[done], tables, spectral, chunks[done][0])

    for index, (low, high) in enumerate(chunks):
        if index == 0:
            waves = by_owner[:, low:high].reshape(-1)
            taken = fourier.at[:, waves, :].get(mode="promise_in_bounds")
            outgoing = jnp.swapaxes(taken, 0, 1).reshape(lat_count, high - low, row_count, column_count)
            outgoing, source, table = lax.optimization_barrier((outgoing, fourier, legendre))
            turned = jnp.swapaxes(source, 0, 1)
            tables, blocks = gather_table(table, lev_count)
            own_waves = lax.dynamic_slice_in_dim(wave_of, lax.axis_index("lat") * slot_count, slot_count)
            parities = jnp.arange(2, dtype=jnp.int32)
            live_count = (wave_count - own_waves[:, None] - parities[None, :] + 1) // 2
            width = max(2, lev_count)
            counts = jnp.zeros((slot_count + 1, width), jnp.int32)
            counts = counts.at[:slot_count, :2].set(live_count)
            counts = counts.at[slot_count, :lev_count].set(jnp.stack(blocks))
        else:
            outgoing = pick_chunk(by_owner, turned, low, high)
        if index == len(chunks) - 1:
            while done < index - 1:
                spectral = project_next(done, spectral)
                done += 1
            if done:
                outgoing, spectral = lax.optimization_barrier((outgoing, spectral))
        arrived = lax.all_to_all(outgoing, "lat", split_axis=0, concat_axis=0, tiled=True)
        if row_count != table_rows:
            arrived = jnp.swapaxes(arrived, 0, 1).reshape(high - low, -1, table_rows, column_count)
            arrived = jnp.swapaxes(arrived, 0, 1)
        arrivals.append(arrived)
    while done < len(chunks):
        spectral = project_next(done, spectral)
        done += 1
    return spectral


def pick_each(wave_ref, *refs):
    count = len(refs) // 2
    for source_ref, out_ref in zip(refs[:count], refs[count:]):
        out_ref[...] = source_ref[...]


def pick_swaps(by_peer, turned, low, high):
    _, rows, columns = turned.shape
    peers = by_peer.shape[0]

    def source_of(peer):
        return pl.BlockSpec((1, rows, columns), lambda step, wave_ref: (wave_ref[peer, low + step], 0, 0))

    out = jax.ShapeDtypeStruct((high - low, rows, columns), turned.dtype)
    return pl.pallas_call(
        pick_each,
        out_shape=[out] * peers,
        grid_spec=pltpu.PrefetchScalarGridSpec(
            num_scalar_prefetch=1,
            grid=(high - low,),
            in_specs=[source_of(peer) for peer in range(peers)],
            out_specs=[pl.BlockSpec((1, rows, columns), lambda step, wave_ref: (step, 0, 0))] * peers,
        ),
        cost_estimate=pl.CostEstimate(flops=0, transcendentals=0, bytes_accessed=4 * peers * out.size),
    )(by_peer, *[turned] * peers)


def stack_blocks(places_ref, *refs):
    out_ref = refs[-1]
    _, parities, rows, _ = refs[0].shape
    for index, table_ref in enumerate(refs[:-1]):
        first_row = pl.multiple_of(places_ref[index] * rows, rows)
        for parity in range(parities):
            out_ref[0, parity, pl.ds(first_row, rows), :] = table_ref[0, parity]


def stack_tables(places, tables):
    slot_count, parities, rows, degrees = tables[0].shape
    whole = (1, parities, rows * len(tables), degrees)
    out = jax.ShapeDtypeStruct((slot_count, *whole[1:]), tables[0].dtype)
    return pl.pallas_call(
        stack_blocks,
        out_shape=out,
        grid_spec=pltpu.PrefetchScalarGridSpec(
            num_scalar_prefetch=1,
            grid=(slot_count,),
            in_specs=[pl.BlockSpec((1, parities, rows, degrees), lambda i, places: (i, 0, 0, 0))] * len(tables),
            out_specs=pl.BlockSpec(whole, lambda i, places: (i, 0, 0, 0)),
        ),
        cost_estimate=pl.CostEstimate(flops=0, transcendentals=0, bytes_accessed=4 * out.size),
    )(places, *tables)


def project_swapped(first_slot, peers, counts_ref, *refs):
    same_refs = refs[: peers // 2]
    other_refs = refs[peers // 2 : peers]
    table_ref = refs[peers]
    out_ref = refs[-1]
    group = out_ref.shape[0]
    sign = counts_ref[counts_ref.shape[0] - 1, 0].astype(jnp.float32).astype(jnp.bfloat16)
    for place in range(group):
        slot = first_slot + pl.program_id(0) * group + place
        same = [ref[place] for ref in same_refs]
        other = [ref[place] for ref in other_refs]
        for parity in range(2):
            if parity == 0:
                parts = [near + far for near, far in zip(same, other)]
            else:
                parts = [(near - far) * sign for near, far in zip(same, other)]
            total = lax.dot_general(
                table_ref[place, parity],
                jnp.concatenate(parts, axis=0),
                (((0,), (0,)), ((), ())),
                preferred_element_type=jnp.float32,
            )
            degree = lax.broadcasted_iota(jnp.int32, total.shape, 0)
            kept = jnp.where(degree < counts_ref[slot, parity], total, 0.0)
            out_ref[place, parity] = kept.astype(out_ref.dtype)


def project_swaps(counts, arrived, table, spectral, first_slot):
    chunk, rows, columns = arrived[0].shape
    slot_count, parities, table_rows, degrees = table.shape
    group = PROJECT_GROUP
    first_group = first_slot // group
    in_specs = [pl.BlockSpec((group, rows, columns), lambda i, counts: (i, 0, 0)) for _ in arrived]
    in_specs.append(
        pl.BlockSpec((group, parities, table_rows, degrees), lambda i, counts: (first_group + i, 0, 0, 0))
    )
    operands = [counts, *arrived, table]
    aliases = {}
    if spectral is not None:
        in_specs.append(pl.BlockSpec(memory_space=pl.ANY))
        aliases = {len(operands): 0}
        operands.append(spectral)
    flops = 2 * chunk * parities * table_rows * degrees * columns
    moved = 2 * chunk * (len(arrived) * rows * columns + parities * degrees * (table_rows + columns))
    return pl.pallas_call(
        functools.partial(project_swapped, first_slot, len(arrived)),
        out_shape=jax.ShapeDtypeStruct((slot_count, parities, degrees, columns), jnp.bfloat16),
        grid_spec=pltpu.PrefetchScalarGridSpec(
            num_scalar_prefetch=1,
            grid=(chunk // group,),
            in_specs=in_specs,
            out_specs=pl.BlockSpec(
                (group, parities, degrees, columns), lambda i, counts: (first_group + i, 0, 0, 0)
            ),
        ),
        input_output_aliases=aliases,
        cost_estimate=pl.CostEstimate(flops=flops, transcendentals=0, bytes_accessed=moved),
    )(*operands)


def swap_order(peers):
    return [*range(peers // 2, peers), *range(1, peers // 2)]


def swap_body(fourier, legendre, owner):
    peers = lax.axis_size("lat")
    lev_count = lax.axis_size("lev")
    row_count, wave_count, column_count = fourier.shape
    slot_count = wave_count // peers
    here = lax.axis_index("lat")
    wave_of = slot_waves(owner, slot_count)
    by_peer = jnp.take(
        wave_of.reshape(peers, slot_count), here ^ jnp.arange(peers), axis=0, mode="clip"
    )
    bounds = chunk_bounds(slot_count, SWAP_ENDS)
    chunks = list(zip(bounds[:-1], bounds[1:]))
    own_waves = by_peer[0]
    parities = jnp.arange(2, dtype=jnp.int32)
    live_count = (wave_count - own_waves[:, None] - parities[None, :] + 1) // 2
    sign = jnp.where(here < peers // 2, 1, -1).astype(jnp.int32)
    counts = jnp.concatenate([live_count, jnp.full((1, 2), sign, jnp.int32)], axis=0)
    arrivals = []
    spectral = None
    stacked = None
    done = 0

    def project_next(done, spectral):
        return project_swaps(counts, arrivals[done], stacked, spectral, bounds[done])

    for index, (low, high) in enumerate(chunks):
        if index == 0:
            waves = by_peer[:, low:high].reshape(-1)
            taken = fourier.at[:, waves, :].get(mode="promise_in_bounds")
            taken = jnp.swapaxes(taken, 0, 1).reshape(peers, high - low, row_count, column_count)
            outgoing = [taken[peer] for peer in range(peers)]
            *outgoing, source, table = lax.optimization_barrier((*outgoing, fourier, legendre))
            turned = jnp.swapaxes(source, 0, 1)
            tables = [table, partner(table, lev_count // 2, lev_count)]
        else:
            outgoing = pick_swaps(by_peer, turned, low, high)
        if index >= 2:
            settled = arrivals[index - 2]
            outgoing = list(lax.optimization_barrier((*outgoing, *settled))[:peers])
        arrived = list(outgoing)
        for distance in swap_order(peers):
            pairs = [(place, place ^ distance) for place in range(peers)]
            arrived[distance] = lax.ppermute(outgoing[distance], "lat", pairs)
        arrivals.append(arrived)
    offsets = [0, lev_count // 2]
    distance = lev_count // 4
    while distance:
        tables += [partner(piece, distance, lev_count) for piece in tables]
        offsets += [offset ^ distance for offset in offsets]
        distance //= 2
    base = lax.axis_index("lev") ^ (here % lev_count)
    stacked = stack_tables(jnp.stack([base ^ offset for offset in offsets]), tables)
    while done < len(chunks):
        spectral = project_next(done, spectral)
        done += 1
    return spectral


def swaps_fit(lat_count, lev_count, fourier_shape, table_shape):
    paired = lat_count == 2 * lev_count and lev_count == 4
    return paired and fourier_shape[0] == table_shape[2] and fourier_shape[1] % (lat_count * SWAP_ENDS[-1]) == 0


def body(fourier, legendre, owner):
    if swaps_fit(lax.axis_size("lat"), lax.axis_size("lev"), fourier.shape, legendre.shape):
        return swap_body(fourier, legendre, owner)
    return exchange_body(fourier, legendre, owner)


def solution(mesh):
    placed = (P("lat", None, "lev"), P("lat", None, "lev", None), P())
    return jax.shard_map(
        body, mesh=mesh, in_specs=placed, out_specs=P("lat", None, None, "lev"), check_vma=False
    )
```

```python
import functools

import jax
import jax.numpy as jnp
from jax import lax
from jax.experimental import pallas as pl
from jax.experimental.pallas import tpu as pltpu
from jax.sharding import PartitionSpec as P


CHUNK_ENDS = (5, 22, 74, 80)
SWAP_ENDS = (4, 10, 58, 74, 78, 80)
PROJECT_GROUP = 2
PICK_GROUP = 4
DEGREE_BLOCK = 128


def slot_waves(owner, slot_count):
    wave_count = owner.shape[0]
    wave_ids = jnp.arange(wave_count, dtype=jnp.int32)
    earlier = (owner[None, :] == owner[:, None]) & (wave_ids[None, :] < wave_ids[:, None])
    ranked = jnp.sum(earlier.astype(jnp.int32), axis=1)
    placed = owner * slot_count + ranked
    matched = placed[None, :] == wave_ids[:, None]
    return jnp.sum(jnp.where(matched, wave_ids[None, :], 0), axis=1)


def chunk_bounds(slot_count, chunk_ends=CHUNK_ENDS):
    ends = {slot_count * end // chunk_ends[-1] for end in chunk_ends}
    return sorted(ends | {0})


def pick(wave_ref, *refs):
    out_ref = refs[-1]
    for place, source_ref in enumerate(refs[:-1]):
        out_ref[0, place] = source_ref[0]


def pick_chunk(by_owner, turned, low, high):
    _, rows, columns = turned.shape
    lat_count = by_owner.shape[0]
    chunk = high - low
    group = min(chunk, PICK_GROUP)
    last_wave = by_owner.shape[1] - 1

    def source_of(place):
        def place_of(owner, step, wave_ref):
            slot = jnp.minimum(low + step * group + place, last_wave)
            return wave_ref[owner, slot], 0, 0

        return pl.BlockSpec((1, rows, columns), place_of)

    out = jax.ShapeDtypeStruct((lat_count, chunk, rows, columns), turned.dtype)
    return pl.pallas_call(
        pick,
        out_shape=out,
        grid_spec=pltpu.PrefetchScalarGridSpec(
            num_scalar_prefetch=1,
            grid=(lat_count, pl.cdiv(chunk, group)),
            in_specs=[source_of(place) for place in range(group)],
            out_specs=pl.BlockSpec((1, group, rows, columns), lambda owner, step, wave: (owner, step, 0, 0)),
        ),
        cost_estimate=pl.CostEstimate(flops=0, transcendentals=0, bytes_accessed=4 * out.size),
    )(by_owner, *[turned] * group)


def project(first_slot, counts_ref, source_ref, *rest):
    groups, _, _, columns = source_ref.shape
    half_groups = groups // 2
    table_refs = rest[:half_groups]
    out_ref = rest[-1]
    _, _, _, degrees = table_refs[0].shape
    slot = first_slot + pl.program_id(0)
    upper, lower = [], []
    for place in range(half_groups):
        block = counts_ref[counts_ref.shape[0] - 1, place]
        upper.append(source_ref[block, 0].astype(jnp.float32))
        lower.append(source_ref[half_groups + block, 0].astype(jnp.float32))
    for parity in range(2):
        pairs = zip(upper, lower)
        parts = [north + south if parity == 0 else north - south for north, south in pairs]
        source = jnp.concatenate([part.astype(jnp.bfloat16) for part in parts], axis=0)
        live = counts_ref[slot, parity]
        for low in range(0, degrees, DEGREE_BLOCK):
            high = min(low + DEGREE_BLOCK, degrees)

            @pl.when(live > low)
            def _(low=low, high=high, source=source, live=live, parity=parity):
                tile = jnp.concatenate([ref[0, parity, :, low:high] for ref in table_refs], axis=0)
                total = lax.dot_general(
                    tile, source, (((0,), (0,)), ((), ())), preferred_element_type=jnp.float32
                )
                degree = low + lax.broadcasted_iota(jnp.int32, total.shape, 0)
                out_ref[0, parity, low:high, :] = jnp.where(degree < live, total, 0.0).astype(out_ref.dtype)

            @pl.when(live <= low)
            def _(low=low, high=high, parity=parity):
                out_ref[0, parity, low:high, :] = jnp.zeros((high - low, columns), out_ref.dtype)


def project_chunk(counts, arrived, tables, spectral, first_slot):
    groups, chunk, rows, columns = arrived.shape
    slot_count, parities, table_rows, degrees = tables[0].shape
    in_specs = [pl.BlockSpec((groups, 1, rows, columns), lambda i, counts: (0, i, 0, 0))]
    for _ in tables:
        in_specs.append(
            pl.BlockSpec((1, parities, table_rows, degrees), lambda i, counts: (first_slot + i, 0, 0, 0))
        )
    operands = [counts, arrived, *tables]
    aliases = {}
    if spectral is not None:
        in_specs.append(pl.BlockSpec(memory_space=pl.ANY))
        aliases = {len(operands): 0}
        operands.append(spectral)
    flops = 2 * chunk * parities * len(tables) * table_rows * degrees * columns
    return pl.pallas_call(
        functools.partial(project, first_slot),
        out_shape=jax.ShapeDtypeStruct((slot_count, parities, degrees, columns), jnp.bfloat16),
        grid_spec=pltpu.PrefetchScalarGridSpec(
            num_scalar_prefetch=1,
            grid=(chunk,),
            in_specs=in_specs,
            out_specs=pl.BlockSpec(
                (1, parities, degrees, columns), lambda i, counts: (first_slot + i, 0, 0, 0)
            ),
        ),
        input_output_aliases=aliases,
        cost_estimate=pl.CostEstimate(flops=flops, transcendentals=0, bytes_accessed=4 * arrived.size),
    )(*operands)


def partner(values, distance, count):
    return lax.ppermute(values, "lev", [(place, place ^ distance) for place in range(count)])


def gather_table(legendre, count):
    tables = [legendre]
    distance = count // 2
    while distance:
        tables += [partner(table, distance, count) for table in tables]
        distance //= 2
    offsets = [0]
    distance = count // 2
    while distance:
        offsets += [offset ^ distance for offset in offsets]
        distance //= 2
    return tables, [lax.axis_index("lev") ^ offset for offset in offsets]


def exchange_body(fourier, legendre, owner):
    lat_count = lax.axis_size("lat")
    lev_count = lax.axis_size("lev")
    row_count, wave_count, column_count = fourier.shape
    slot_count = wave_count // lat_count
    table_rows = legendre.shape[2]
    wave_of = slot_waves(owner, slot_count)
    by_owner = wave_of.reshape(lat_count, slot_count)
    bounds = chunk_bounds(slot_count)
    chunks = list(zip(bounds[:-1], bounds[1:]))
    turned = None
    arrivals = []
    spectral = None
    done = 0

    def project_next(done, spectral):
        return project_chunk(counts, arrivals[done], tables, spectral, chunks[done][0])

    for index, (low, high) in enumerate(chunks):
        if index == 0:
            waves = by_owner[:, low:high].reshape(-1)
            taken = fourier.at[:, waves, :].get(mode="promise_in_bounds")
            outgoing = jnp.swapaxes(taken, 0, 1).reshape(lat_count, high - low, row_count, column_count)
            outgoing, source, table = lax.optimization_barrier((outgoing, fourier, legendre))
            turned = jnp.swapaxes(source, 0, 1)
            tables, blocks = gather_table(table, lev_count)
            own_waves = lax.dynamic_slice_in_dim(wave_of, lax.axis_index("lat") * slot_count, slot_count)
            parities = jnp.arange(2, dtype=jnp.int32)
            live_count = (wave_count - own_waves[:, None] - parities[None, :] + 1) // 2
            width = max(2, lev_count)
            counts = jnp.zeros((slot_count + 1, width), jnp.int32)
            counts = counts.at[:slot_count, :2].set(live_count)
            counts = counts.at[slot_count, :lev_count].set(jnp.stack(blocks))
        else:
            outgoing = pick_chunk(by_owner, turned, low, high)
        if index == len(chunks) - 1:
            while done < index - 1:
                spectral = project_next(done, spectral)
                done += 1
            if done:
                outgoing, spectral = lax.optimization_barrier((outgoing, spectral))
        arrived = lax.all_to_all(outgoing, "lat", split_axis=0, concat_axis=0, tiled=True)
        if row_count != table_rows:
            arrived = jnp.swapaxes(arrived, 0, 1).reshape(high - low, -1, table_rows, column_count)
            arrived = jnp.swapaxes(arrived, 0, 1)
        arrivals.append(arrived)
    while done < len(chunks):
        spectral = project_next(done, spectral)
        done += 1
    return spectral


def pick_each(wave_ref, *refs):
    count = len(refs) // 2
    for source_ref, out_ref in zip(refs[:count], refs[count:]):
        out_ref[...] = source_ref[...]


def pick_swaps(by_peer, turned, low, high):
    _, rows, columns = turned.shape
    peers = by_peer.shape[0]

    def source_of(peer):
        return pl.BlockSpec((1, rows, columns), lambda step, wave_ref: (wave_ref[peer, low + step], 0, 0))

    out = jax.ShapeDtypeStruct((high - low, rows, columns), turned.dtype)
    return pl.pallas_call(
        pick_each,
        out_shape=[out] * peers,
        grid_spec=pltpu.PrefetchScalarGridSpec(
            num_scalar_prefetch=1,
            grid=(high - low,),
            in_specs=[source_of(peer) for peer in range(peers)],
            out_specs=[pl.BlockSpec((1, rows, columns), lambda step, wave_ref: (step, 0, 0))] * peers,
        ),
        cost_estimate=pl.CostEstimate(flops=0, transcendentals=0, bytes_accessed=4 * peers * out.size),
    )(by_peer, *[turned] * peers)


def stack_blocks(places_ref, *refs):
    out_ref = refs[-1]
    _, parities, rows, _ = refs[0].shape
    for index, table_ref in enumerate(refs[:-1]):
        first_row = pl.multiple_of(places_ref[index] * rows, rows)
        for parity in range(parities):
            out_ref[0, parity, pl.ds(first_row, rows), :] = table_ref[0, parity]


def stack_tables(places, tables):
    slot_count, parities, rows, degrees = tables[0].shape
    whole = (1, parities, rows * len(tables), degrees)
    out = jax.ShapeDtypeStruct((slot_count, *whole[1:]), tables[0].dtype)
    return pl.pallas_call(
        stack_blocks,
        out_shape=out,
        grid_spec=pltpu.PrefetchScalarGridSpec(
            num_scalar_prefetch=1,
            grid=(slot_count,),
            in_specs=[pl.BlockSpec((1, parities, rows, degrees), lambda i, places: (i, 0, 0, 0))] * len(tables),
            out_specs=pl.BlockSpec(whole, lambda i, places: (i, 0, 0, 0)),
        ),
        cost_estimate=pl.CostEstimate(flops=0, transcendentals=0, bytes_accessed=4 * out.size),
    )(places, *tables)


def project_swapped(first_slot, peers, counts_ref, *refs):
    same_refs = refs[: peers // 2]
    other_refs = refs[peers // 2 : peers]
    table_ref = refs[peers]
    out_ref = refs[-1]
    group = out_ref.shape[0]
    sign = counts_ref[counts_ref.shape[0] - 1, 0].astype(jnp.float32).astype(jnp.bfloat16)
    for place in range(group):
        slot = first_slot + pl.program_id(0) * group + place
        same = [ref[place] for ref in same_refs]
        other = [ref[place] for ref in other_refs]
        for parity in range(2):
            if parity == 0:
                parts = [near + far for near, far in zip(same, other)]
            else:
                parts = [(near - far) * sign for near, far in zip(same, other)]
            total = lax.dot_general(
                table_ref[place, parity],
                jnp.concatenate(parts, axis=0),
                (((0,), (0,)), ((), ())),
                preferred_element_type=jnp.float32,
            )
            degree = lax.broadcasted_iota(jnp.int32, total.shape, 0)
            kept = jnp.where(degree < counts_ref[slot, parity], total, 0.0)
            out_ref[place, parity] = kept.astype(out_ref.dtype)


def project_swaps(counts, arrived, table, spectral, first_slot):
    chunk, rows, columns = arrived[0].shape
    slot_count, parities, table_rows, degrees = table.shape
    group = PROJECT_GROUP
    first_group = first_slot // group
    in_specs = [pl.BlockSpec((group, rows, columns), lambda i, counts: (i, 0, 0)) for _ in arrived]
    in_specs.append(
        pl.BlockSpec((group, parities, table_rows, degrees), lambda i, counts: (first_group + i, 0, 0, 0))
    )
    operands = [counts, *arrived, table]
    aliases = {}
    if spectral is not None:
        in_specs.append(pl.BlockSpec(memory_space=pl.ANY))
        aliases = {len(operands): 0}
        operands.append(spectral)
    flops = 2 * chunk * parities * table_rows * degrees * columns
    moved = 2 * chunk * (len(arrived) * rows * columns + parities * degrees * (table_rows + columns))
    return pl.pallas_call(
        functools.partial(project_swapped, first_slot, len(arrived)),
        out_shape=jax.ShapeDtypeStruct((slot_count, parities, degrees, columns), jnp.bfloat16),
        grid_spec=pltpu.PrefetchScalarGridSpec(
            num_scalar_prefetch=1,
            grid=(chunk // group,),
            in_specs=in_specs,
            out_specs=pl.BlockSpec(
                (group, parities, degrees, columns), lambda i, counts: (first_group + i, 0, 0, 0)
            ),
        ),
        input_output_aliases=aliases,
        cost_estimate=pl.CostEstimate(flops=flops, transcendentals=0, bytes_accessed=moved),
    )(*operands)


def swap_order(peers):
    return [*range(peers // 2, peers), *range(1, peers // 2)]


def swap_body(fourier, legendre, owner):
    peers = lax.axis_size("lat")
    lev_count = lax.axis_size("lev")
    row_count, wave_count, column_count = fourier.shape
    slot_count = wave_count // peers
    here = lax.axis_index("lat")
    wave_of = slot_waves(owner, slot_count)
    by_peer = jnp.take(
        wave_of.reshape(peers, slot_count), here ^ jnp.arange(peers), axis=0, mode="clip"
    )
    bounds = chunk_bounds(slot_count, SWAP_ENDS)
    chunks = list(zip(bounds[:-1], bounds[1:]))
    own_waves = by_peer[0]
    parities = jnp.arange(2, dtype=jnp.int32)
    live_count = (wave_count - own_waves[:, None] - parities[None, :] + 1) // 2
    sign = jnp.where(here < peers // 2, 1, -1).astype(jnp.int32)
    counts = jnp.concatenate([live_count, jnp.full((1, 2), sign, jnp.int32)], axis=0)
    arrivals = []
    spectral = None
    stacked = None
    done = 0

    def project_next(done, spectral):
        return project_swaps(counts, arrivals[done], stacked, spectral, bounds[done])

    for index, (low, high) in enumerate(chunks):
        if index == 0:
            waves = by_peer[:, low:high].reshape(-1)
            taken = fourier.at[:, waves, :].get(mode="promise_in_bounds")
            taken = jnp.swapaxes(taken, 0, 1).reshape(peers, high - low, row_count, column_count)
            outgoing = [taken[peer] for peer in range(peers)]
            final = swap_order(peers)[-1]
            tied = lax.optimization_barrier((outgoing[final], fourier, legendre))
            outgoing[final], source, table = tied
            turned = jnp.swapaxes(source, 0, 1)
            tables = [table, partner(table, lev_count // 2, lev_count)]
        else:
            outgoing = pick_swaps(by_peer, turned, low, high)
        if index >= 2:
            settled = arrivals[index - 2]
            outgoing = list(lax.optimization_barrier((*outgoing, *settled))[:peers])
        arrived = list(outgoing)
        for distance in swap_order(peers):
            pairs = [(place, place ^ distance) for place in range(peers)]
            arrived[distance] = lax.ppermute(outgoing[distance], "lat", pairs)
        arrivals.append(arrived)
    offsets = [0, lev_count // 2]
    distance = lev_count // 4
    while distance:
        tables += [partner(piece, distance, lev_count) for piece in tables]
        offsets += [offset ^ distance for offset in offsets]
        distance //= 2
    base = lax.axis_index("lev") ^ (here % lev_count)
    stacked = stack_tables(jnp.stack([base ^ offset for offset in offsets]), tables)
    while done < len(chunks):
        spectral = project_next(done, spectral)
        done += 1
    return spectral


def swaps_fit(lat_count, lev_count, fourier_shape, table_shape):
    paired = lat_count == 2 * lev_count and lev_count == 4
    return paired and fourier_shape[0] == table_shape[2] and fourier_shape[1] % (lat_count * SWAP_ENDS[-1]) == 0


def body(fourier, legendre, owner):
    if swaps_fit(lax.axis_size("lat"), lax.axis_size("lev"), fourier.shape, legendre.shape):
        return swap_body(fourier, legendre, owner)
    return exchange_body(fourier, legendre, owner)


def solution(mesh):
    placed = (P("lat", None, "lev"), P("lat", None, "lev", None), P())
    return jax.shard_map(
        body, mesh=mesh, in_specs=placed, out_specs=P("lat", None, None, "lev"), check_vma=False
    )
```
